8 devices in a mesh: dp: 2 (over y, z), tp: 4 (over x, core).
Axes of the slice: x: 2, y: 2, z: 1, core: 2. Of those that a mesh axis runs over, the one named last changes fastest.
Arguments:
- x: bfloat16 [4096, 2048], P('dp'), parts along dimension 0
- w_gate: bfloat16 [2048, 8192], P(None, 'tp')
- w_up: bfloat16 [2048, 8192], P(None, 'tp')
- w_down: bfloat16 [8192, 2048], P('tp')
Outputs:
- output: bfloat16 [4096, 2048], P('dp'), parts along dimension 0
There are 2 independent parts. The reference program is written for one: setup_inputs(seed, part) draws one part's arguments, and reference() takes and returns one part's arrays. A program takes and returns all parts, laid end to end along the dimension named above; an argument that names none is the same for every part.
All inputs are finite; a program needn't handle non-finite values.
Results may differ from the reference program's by a relative error of at most 0.016.
Values are sent between devices in bfloat16 or wider.
A program may use at most 2 GiB of HBM per device.

```python
import jax
import jax.numpy as jnp

ROWS = 2048
D = 2048
FF = 8192


def setup_inputs(seed: int = 0, part: int = 0) -> dict:
    kx, kg, ku, kd = jax.random.split(jax.random.key(seed), 4)
    drawn = {
        "x": jax.random.normal(jax.random.fold_in(kx, part), (ROWS, D), jnp.float32),
        "w_gate": jax.random.normal(kg, (D, FF), jnp.float32) * D**-0.5,
        "w_up": jax.random.normal(ku, (D, FF), jnp.float32) * D**-0.5,
        "w_down": jax.random.normal(kd, (FF, D), jnp.float32) * FF**-0.5,
    }
    return {k: v.astype(jnp.bfloat16) for k, v in drawn.items()}


def reference(x, w_gate, w_up, w_down):
    gate = jnp.dot(x, w_gate, preferred_element_type=jnp.float32)
    up = jnp.dot(x, w_up, preferred_element_type=jnp.float32)
    hidden = (jax.nn.silu(gate) * up).astype(jnp.bfloat16)
    return jnp.dot(hidden, w_down, preferred_element_type=jnp.float32).astype(jnp.bfloat16)
```

```python
import functools

import jax
import jax.numpy as jnp
from jax import lax
from jax.experimental import pallas as pl
from jax.experimental.pallas import tpu as pltpu
from jax.sharding import PartitionSpec as P

MESH = pl.DeviceIdType.MESH
BF16, F32 = jnp.bfloat16, jnp.float32
R = 256
C = 256


def kernel(
    n, x_hbm, wg_hbm, wu_hbm, wd_hbm, y, xb, wg, wu, wd, h, t_send, t_recv, rs_send, rs_recv, own,
    x_sem, w_sem, d_sem, ts_sem, tr_sem, rss_sem, rsr_sem, ags_sem, agr_sem, fs_sem, fr_sem, gs_sem, gr_sem,
):
    me = lax.axis_index("tp")
    a, c = me // 2, lax.rem(me, 2)
    sib = {"tp": me + 1 - 2 * c}
    across = {"tp": lax.rem(me + 2, 4)}
    tiles = wg.shape[0]

    def column(half, quarter, i):
        return pl.multiple_of(half * 4 * C + quarter * 2 * C + i * C, C)

    def at(ref, k, col):
        return ref.at[pl.ds(pl.multiple_of(k * R, R), R), pl.ds(col, C)]

    def down_column(u):
        half = 1 - c if u < 4 else c
        return column(half, 1 - a if u % 4 < 2 else a, u % 2)

    def load_x(k):
        return pltpu.make_async_copy(
            x_hbm.at[pl.ds(pl.multiple_of(k * R, R), R), :], xb.at[lax.rem(k, 2)], x_sem.at[lax.rem(k, 2)]
        )

    def load_w(j):
        cols = pl.ds(pl.multiple_of(j * C, C), C)
        return (
            pltpu.make_async_copy(wg_hbm.at[:, cols], wg.at[j], w_sem.at[0, j]),
            pltpu.make_async_copy(wu_hbm.at[:, cols], wu.at[j], w_sem.at[1, j]),
        )

    def load_d(u):
        return pltpu.make_async_copy(wd_hbm.at[:, pl.ds(down_column(u), C)], wd.at[u], d_sem.at[u])

    def remote(src, dst, ssem, rsem, to):
        return pltpu.make_async_remote_copy(src, dst, ssem, rsem, device_id=to, device_id_type=MESH)

    def term_copy(k, u):
        s = lax.rem(k, 2)
        return remote(t_send.at[s, u], t_recv.at[k, u], ts_sem.at[s, u], tr_sem.at[k, u], sib)

    def rs_copy(k, i):
        return remote(rs_send.at[k, i], rs_recv.at[k, i], rss_sem.at[k, i], rsr_sem.at[k, i], across)

    def ag_copy(k, i):
        part = at(y, k, column(c, a, i))
        return remote(part, part, ags_sem.at[k, i], agr_sem.at[k, i], across)

    def own_copy(k, i):
        part = at(y, k, column(c, a, i))
        return remote(part, part, fs_sem.at[k, i], fr_sem.at[k, i], sib)

    def pass_copy(k, i):
        part = at(y, k, column(c, 1 - a, i))
        return remote(part, part, gs_sem.at[k, i], gr_sem.at[k, i], sib)

    barrier = pltpu.get_barrier_semaphore()
    for to in (sib, across):
        pl.semaphore_signal(barrier, inc=1, device_id=to, device_id_type=MESH)

    load_x(0).start()
    for j in range(3):
        for copy in load_w(j):
            copy.start()

    def finish(k):
        for i in range(2):
            rs_copy(k, i).wait_recv()
            col = column(c, a, i)
            y[pl.ds(pl.multiple_of(k * R, R), R), pl.ds(col, C)] = (own[k, i] + rs_recv[k, i].astype(F32)).astype(BF16)
            ag_copy(k, i).start()
            own_copy(k, i).start()

    def chunk(k, first=False):
        slot = lax.rem(k, 2)

        @pl.when(k + 1 < n)
        def _():
            load_x(k + 1).start()

        load_x(k).wait()

        @pl.loop(0, tiles)
        def _(j):
            if first:
                @pl.when(j + 3 < tiles)
                def _():
                    for copy in load_w(j + 3):
                        copy.start()

                for s in range(3):
                    @pl.when(j == tiles - 3 + s)
                    def _():
                        for u in range(2 * s, 2 * s + 2 if s < 2 else 8):
                            load_d(u).start()

                for copy in load_w(j):
                    copy.wait()

            gate = jnp.dot(xb[slot], wg[j], preferred_element_type=F32)
            up = jnp.dot(xb[slot], wu[j], preferred_element_type=F32)
            h[:, pl.ds(pl.multiple_of(j * C, C), C)] = (jax.nn.silu(gate) * up).astype(BF16)

        if first:
            for u in range(8):
                load_d(u).wait()
            pl.semaphore_wait(barrier, 2)
        else:
            @pl.when(lax.rem(k, 3) != 2)
            def _():
                finish((2 * k + 1) // 3 - 1)

        @pl.loop(0, 4)
        def _(u):
            @pl.when(k >= 2)
            def _():
                term_copy(k, u).wait_send()

            t_send[slot, u] = jnp.dot(h[...], wd[u], preferred_element_type=F32).astype(BF16)
            term_copy(k, u).start()

        @pl.loop(0, 2)
        def _(i):
            term = jnp.dot(h[...], wd[4 + i], preferred_element_type=F32)
            term_copy(k, i).wait_recv()
            rs_send[k, i] = (term + t_recv[k, i].astype(F32)).astype(BF16)
            rs_copy(k, i).start()

        @pl.loop(0, 2)
        def _(i):
            term = jnp.dot(h[...], wd[6 + i], preferred_element_type=F32)
            term_copy(k, 2 + i).wait_recv()
            own[k, i] = term + t_recv[k, 2 + i].astype(F32)

    chunk(0, first=True)

    @pl.loop(1, n)
    def _(k):
        chunk(k)

    @pl.loop((2 * n - 1) // 3, n)
    def _(k):
        finish(k)

    @pl.loop(0, n)
    def _(k):
        for i in range(2):
            ag_copy(k, i).wait_recv()
            pass_copy(k, i).start()

    @pl.loop(0, n)
    def _(k):
        for i in range(2):
            own_copy(k, i).wait_recv()
            rs_copy(k, i).wait_send()
            ag_copy(k, i).wait_send()
            own_copy(k, i).wait_send()

    for s in range(2):
        for u in range(4):
            term_copy(s, u).wait_send()

    @pl.loop(0, n)
    def _(k):
        for i in range(2):
            pass_copy(k, i).wait()


def put_kernel(y_vmem, out, sem):
    copy = pltpu.make_async_copy(y_vmem, out, sem)
    copy.start()
    copy.wait()


def solution(mesh):
    def step(x, w_gate, w_up, w_down):
        rows, d = x.shape
        ff = w_gate.shape[1]
        n, tiles = rows // R, ff // C
        dma = pltpu.SemaphoreType.DMA
        y = pl.pallas_call(
            functools.partial(kernel, n),
            out_shape=pltpu.VMEM((rows, d), BF16),
            in_specs=[pl.BlockSpec(memory_space=pltpu.HBM)] * 4,
            out_specs=pl.BlockSpec(memory_space=pltpu.VMEM),
            scratch_shapes=[
                pltpu.VMEM((2, R, d), BF16),
                pltpu.VMEM((tiles, d, C), BF16),
                pltpu.VMEM((tiles, d, C), BF16),
                pltpu.VMEM((8, ff, C), BF16),
                pltpu.VMEM((R, ff), BF16),
                pltpu.VMEM((2, 4, R, C), BF16),
                pltpu.VMEM((n, 4, R, C), BF16),
                pltpu.VMEM((n, 2, R, C), BF16),
                pltpu.VMEM((n, 2, R, C), BF16),
                pltpu.VMEM((n, 2, R, C), F32),
                dma((2,)), dma((2, tiles)), dma((8,)),
                dma((2, 4)), dma((n, 4)), dma((n, 2)), dma((n, 2)), dma((n, 2)), dma((n, 2)),
                dma((n, 2)), dma((n, 2)), dma((n, 2)), dma((n, 2)),
            ],
            compiler_params=pltpu.CompilerParams(
                collective_id=0, has_side_effects=True, vmem_limit_bytes=52 * 2**20
            ),
            cost_estimate=pl.CostEstimate(
                flops=6 * rows * d * ff, bytes_accessed=2 * (2 * rows * d + 3 * d * ff), transcendentals=rows * ff
            ),
        )(x, w_gate, w_up, w_down)
        return y

    return jax.shard_map(
        step,
        mesh=mesh,
        in_specs=(P("dp", None), P(None, "tp"), P(None, "tp"), P("tp", None)),
        out_specs=P("dp", None),
        check_vma=False,
    )
```

```python
import functools

import jax
import jax.numpy as jnp
from jax import lax
from jax.experimental import pallas as pl
from jax.experimental.pallas import tpu as pltpu
from jax.sharding import PartitionSpec as P

MESH = pl.DeviceIdType.MESH
BF16, F32 = jnp.bfloat16, jnp.float32
R = 256
C = 256
AHEAD = 3
LAST = 2


def kernel(
    n, x_hbm, wg_hbm, wu_hbm, wd_hbm, y, xb, wgu, wd, h, t_send, t_recv, cross, rs_send, rs_recv, own,
    x_sem, w_sem, d_sem, ts_sem, tr_sem, ta_sem, rss_sem, rsr_sem, ags_sem, agr_sem, fs_sem, gs_sem, yr_sem,
):
    me = lax.axis_index("tp")
    a, c = me // 2, lax.rem(me, 2)
    sib = {"tp": me + 1 - 2 * c}
    across = {"tp": lax.rem(me + 2, 4)}
    tiles = wgu.shape[0]
    rows = n * R

    def column(half, quarter, i):
        return pl.multiple_of(half * 4 * C + quarter * 2 * C + i * C, C)

    def at(ref, k, col, chunks=1, wide=1):
        return ref.at[pl.ds(pl.multiple_of(k * R, R), chunks * R), pl.ds(col, wide * C)]

    def load_x(k):
        return pltpu.make_async_copy(
            x_hbm.at[pl.ds(pl.multiple_of(k * R, R), R), :], xb.at[lax.rem(k, 2)], x_sem.at[lax.rem(k, 2)]
        )

    def start_w(j):
        for m, w in enumerate((wg_hbm, wu_hbm)):
            pltpu.make_async_copy(w.at[:, pl.ds(j * C, C)], wgu.at[j, m], w_sem.at[j % AHEAD]).start(priority=1 if j else 0)

    def wait_w(j):
        pltpu.make_async_copy(wgu.at[j], wgu.at[j], w_sem.at[j % AHEAD]).wait()

    def load_d(u):
        half = 1 - c if u % 4 < 2 else c
        col = column(half, 1 - a if u < 4 else a, u % 2)
        return pltpu.make_async_copy(wd_hbm.at[:, pl.ds(col, C)], wd.at[u], d_sem.at[u // 4])

    def remote(src, dst, ssem, rsem, to):
        return pltpu.make_async_remote_copy(src, dst, ssem, rsem, device_id=to, device_id_type=MESH)

    def cross_term(k, i):
        return remote(t_send.at[k, i], t_recv.at[k, i], ts_sem, tr_sem.at[lax.rem(k, 4), i], sib)

    def own_term(k):
        two = pl.ds(2, 2)
        return remote(t_send.at[k, two], t_recv.at[k, two], ts_sem, ta_sem.at[lax.rem(k, 4)], sib)

    def rs_copy(k, i):
        return remote(rs_send.at[k, i], rs_recv.at[k, i], rss_sem, rsr_sem.at[lax.rem(k, 4), i], across)

    def ag_copy(k, i):
        part = at(y, k, column(c, a, i))
        slot = k // (n - LAST) * (1 + 2 * (k - (n - LAST)) + i)
        return remote(part, part, ags_sem, agr_sem.at[slot], across)

    def own_copy(k, i):
        part = at(y, k, column(c, a, i))
        return remote(part, part, fs_sem, yr_sem, sib)

    def pass_copy(k, i, chunks=1, wide=1):
        part = at(y, k, column(c, 1 - a, i), chunks, wide)
        return remote(part, part, gs_sem, yr_sem, sib)

    def drain(ref, sem):
        pltpu.make_async_copy(ref, ref, sem).wait()

    load_x(0).start()
    for j in range(AHEAD):
        start_w(j)
    barrier = pltpu.get_barrier_semaphore()
    for to in (sib, across):
        pl.semaphore_signal(barrier, inc=1, device_id=to, device_id_type=MESH)

    def down(u, first, count):
        return jnp.dot(h[pl.ds(first, count)], wd[u], preferred_element_type=F32)

    def down_two(us, put):
        parts = [down(u, 0, R) for u in us]
        for i, part in enumerate(parts):
            put(i, slice(None), part)

    def down_one(u, i, put):
        parts = [down(u, half * R // 2, R // 2) for half in range(2)]
        for half, part in enumerate(parts):
            put(i, pl.ds(half * R // 2, R // 2), part)

    def send_cross(k, i):
        cross_term(k, i).wait_recv()
        rs_send[k, i] = (cross[i] + t_recv[k, i].astype(F32)).astype(BF16)
        rs_copy(k, i).start()

    def finish(k, i):
        if i == 0:
            own_term(k).wait_recv()
        rs_copy(k, i).wait_recv()
        total = own[lax.rem(k, 2), i] + t_recv[k, 2 + i].astype(F32) + rs_recv[k, i].astype(F32)
        y[pl.ds(pl.multiple_of(k * R, R), R), pl.ds(column(c, a, i), C)] = total.astype(BF16)
        ag_copy(k, i).start()
        own_copy(k, i).start()

    def chunk(k, first=False):
        slot = lax.rem(k, 2)

        @pl.when(k + 1 < n)
        def _():
            load_x(k + 1).start()

        load_x(k).wait()
        groups = [[j] for j in range(tiles - 2)] + [[tiles - 2, tiles - 1]] if first else [range(tiles)]
        for g, group in enumerate(groups):
            if first:
                for j in group:
                    wait_w(j)
                for j in group:
                    if j + AHEAD < tiles:
                        start_w(j + AHEAD)
                if g >= len(groups) - 2:
                    for u in range(2) if g < len(groups) - 1 else range(2, 4):
                        load_d(u).start()
            for j in group:
                gate = jnp.dot(xb[slot], wgu[j, 0], preferred_element_type=F32)
                up = jnp.dot(xb[slot], wgu[j, 1], preferred_element_type=F32)
                h[:, pl.ds(j * C, C)] = (jax.nn.silu(gate) * up).astype(BF16)

        def put_send(i, part, value):
            t_send[k, i, part] = value.astype(BF16)

        def put_cross(i, part, value):
            cross[i, part] = value

        def put_later(i, part, value):
            t_send[k, 2 + i, part] = value.astype(BF16)

        def put_own(i, part, value):
            own[slot, i, part] = value

        if first:
            for u in range(4, 8):
                load_d(u).start()
            pl.semaphore_wait(barrier, 2)
            drain(wd.at[pl.ds(0, 4)], d_sem.at[0])
            for i in range(2):
                down_one(i, i, put_send)
                cross_term(k, i).start()
            for i in range(2):
                down_one(2 + i, i, put_cross)
                send_cross(k, i)
            drain(wd.at[pl.ds(4, 4)], d_sem.at[1])
        else:
            @pl.when(k == 1)
            def _():
                finish(0, 0)

            down_two((0, 1), put_send)
            for i in range(2):
                cross_term(k, i).start()
            down_two((2, 3), put_cross)
        down_two((4, 5), put_later)
        own_term(k).start()
        down_two((6, 7), put_own)

        if not first:
            for i in range(2):
                send_cross(k, i)

            @pl.when(k > 1)
            def _():
                finish(k - 1, 0)

            finish(k - 1, 1)

    chunk(0, first=True)

    @pl.loop(1, n)
    def _(k):
        chunk(k)

    for i in range(2):
        finish(n - 1, i)

    bulk = at(y, 0, column(c, 1 - a, 0), n - LAST, 2)
    drain(bulk, agr_sem.at[0])
    pass_copy(0, 0, n - LAST, 2).start()
    for k in range(n - LAST, n):
        for i in range(2):
            ag_copy(k, i).wait_recv()
            pass_copy(k, i).start()

    drain(t_send, ts_sem)
    drain(rs_send, rss_sem)
    mine = at(y, 0, column(c, a, 0), n, 2)
    drain(mine, ags_sem)
    drain(mine, fs_sem)
    drain(at(y, 0, column(c, 1 - a, 0), n, 2), gs_sem)
    drain(at(y, 0, column(1 - c, 0, 0), n, 4), yr_sem)


def solution(mesh):
    def step(x, w_gate, w_up, w_down):
        rows, d = x.shape
        ff = w_gate.shape[1]
        n, tiles = rows // R, ff // C
        dma = pltpu.SemaphoreType.DMA
        return pl.pallas_call(
            functools.partial(kernel, n),
            out_shape=pltpu.VMEM((rows, d), BF16),
            in_specs=[pl.BlockSpec(memory_space=pltpu.HBM)] * 4,
            out_specs=pl.BlockSpec(memory_space=pltpu.VMEM),
            scratch_shapes=[
                pltpu.VMEM((2, R, d), BF16),
                pltpu.VMEM((tiles, 2, d, C), BF16),
                pltpu.VMEM((8, ff, C), BF16),
                pltpu.VMEM((R, ff), BF16),
                pltpu.VMEM((n, 4, R, C), BF16),
                pltpu.VMEM((n, 4, R, C), BF16),
                pltpu.VMEM((2, R, C), F32),
                pltpu.VMEM((n, 2, R, C), BF16),
                pltpu.VMEM((n, 2, R, C), BF16),
                pltpu.VMEM((2, 2, R, C), F32),
                dma((2,)), dma((AHEAD,)), dma((2,)), dma(()), dma((4, 2)), dma((4,)), dma(()), dma((4, 2)),
                dma(()), dma((1 + 2 * LAST,)), dma(()), dma(()), dma(()),
            ],
            compiler_params=pltpu.CompilerParams(
                collective_id=0, has_side_effects=True, vmem_limit_bytes=52 * 2**20
            ),
            cost_estimate=pl.CostEstimate(
                flops=6 * rows * d * ff, bytes_accessed=2 * (2 * rows * d + 3 * d * ff), transcendentals=rows * ff
            ),
        )(x, w_gate, w_up, w_down)

    return jax.shard_map(
        step,
        mesh=mesh,
        in_specs=(P("dp", None), P(None, "tp"), P(None, "tp"), P("tp", None)),
        out_specs=P("dp", None),
        check_vma=False,
    )
```

```python
import functools

import jax
import jax.numpy as jnp
from jax import lax
from jax.experimental import pallas as pl
from jax.experimental.pallas import tpu as pltpu
from jax.sharding import PartitionSpec as P

MESH = pl.DeviceIdType.MESH
BF16, F32 = jnp.bfloat16, jnp.float32
R = 256
H = R // 2
C = 256
AHEAD = 3
LAST = 2


def kernel(
    n, x_hbm, wg_hbm, wu_hbm, wd_hbm, y, xb, wgu, wd, h, t_send, t_recv, cross, rs_send, rs_recv, own,
    x_sem, w_sem, d_sem, ts_sem, tr_sem, ta_sem, rss_sem, rsr_sem, ags_sem, agr_sem, fs_sem, gs_sem, yr_sem,
):
    me = lax.axis_index("tp")
    a, c = me // 2, lax.rem(me, 2)
    sib = {"tp": me + 1 - 2 * c}
    across = {"tp": lax.rem(me + 2, 4)}
    tiles = wgu.shape[0]
    rows = n * R

    def column(half, quarter, i):
        return pl.multiple_of(half * 4 * C + quarter * 2 * C + i * C, C)

    def span(half):
        return pl.ds(0, R) if half is None else pl.ds(half * H, H)

    def slot_of(k, half):
        return 4 if half == 1 else lax.rem(k, 4)

    def tile(k, i, half):
        first, count = (0, R) if half is None else (half * H, H)
        return pl.ds(pl.multiple_of(k * R + first, H), count), pl.ds(column(c, a, i), C)

    def at(ref, k, col, chunks=1, wide=1):
        return ref.at[pl.ds(pl.multiple_of(k * R, R), chunks * R), pl.ds(col, wide * C)]

    def load_x(k):
        return pltpu.make_async_copy(
            x_hbm.at[pl.ds(pl.multiple_of(k * R, R), R), :], xb.at[lax.rem(k, 2)], x_sem.at[lax.rem(k, 2)]
        )

    def start_w(j):
        for m, w in enumerate((wg_hbm, wu_hbm)):
            pltpu.make_async_copy(w.at[:, pl.ds(j * C, C)], wgu.at[j, m], w_sem.at[j % AHEAD]).start(priority=1 if j else 0)

    def wait_w(j):
        pltpu.make_async_copy(wgu.at[j], wgu.at[j], w_sem.at[j % AHEAD]).wait()

    def load_d(u):
        half = 1 - c if u % 4 < 2 else c
        col = column(half, 1 - a if u < 4 else a, u % 2)
        return pltpu.make_async_copy(wd_hbm.at[:, pl.ds(col, C)], wd.at[u], d_sem.at[u // 2])

    def remote(src, dst, ssem, rsem, to):
        return pltpu.make_async_remote_copy(src, dst, ssem, rsem, device_id=to, device_id_type=MESH)

    def cross_term(k, i, half):
        part = span(half)
        return remote(
            t_send.at[k, i, part], t_recv.at[k, i, part], ts_sem, tr_sem.at[slot_of(k, half), i], sib
        )

    def own_term(k, half):
        two, part = pl.ds(2, 2), span(half)
        return remote(
            t_send.at[k, two, part], t_recv.at[k, two, part], ts_sem, ta_sem.at[slot_of(k, half)], sib
        )

    def rs_copy(k, i, half):
        part = span(half)
        return remote(
            rs_send.at[k, i, part], rs_recv.at[k, i, part], rss_sem, rsr_sem.at[slot_of(k, half), i], across
        )

    def ag_copy(k, i, half=None):
        part = y.at[tile(k, i, half)]
        slot = k // (n - LAST) * (1 + 2 * (k - (n - LAST)) + i)
        return remote(part, part, ags_sem, agr_sem.at[slot], across)

    def own_copy(k, i, half):
        part = y.at[tile(k, i, half)]
        return remote(part, part, fs_sem, yr_sem, sib)

    def pass_copy(k, i, chunks=1, wide=1):
        part = at(y, k, column(c, 1 - a, i), chunks, wide)
        return remote(part, part, gs_sem, yr_sem, sib)

    def drain(ref, sem):
        pltpu.make_async_copy(ref, ref, sem).wait()

    load_x(0).start()
    for j in range(AHEAD):
        start_w(j)
    barrier = pltpu.get_barrier_semaphore()
    for to in (sib, across):
        pl.semaphore_signal(barrier, inc=1, device_id=to, device_id_type=MESH)

    def send_cross(k, i, half=None):
        part = span(half)
        cross_term(k, i, half).wait_recv()
        rs_send[k, i, part] = (cross[i, part] + t_recv[k, i, part].astype(F32)).astype(BF16)
        rs_copy(k, i, half).start()

    def finish(k, i, half=None):
        part = span(half)
        if i == 0:
            own_term(k, half).wait_recv()
        rs_copy(k, i, half).wait_recv()
        total = own[lax.rem(k, 2), i, part] + t_recv[k, 2 + i, part].astype(F32) + rs_recv[k, i, part].astype(F32)
        y[tile(k, i, half)] = total.astype(BF16)
        ag_copy(k, i, half).start()
        own_copy(k, i, half).start()

    def hidden(k, j, half):
        slot, part = lax.rem(k, 2), span(half)
        rows = xb[slot, part]
        gate = jnp.dot(rows, wgu[j, 0], preferred_element_type=F32)
        up = jnp.dot(rows, wgu[j, 1], preferred_element_type=F32)
        h[part, pl.ds(j * C, C)] = (jax.nn.silu(gate) * up).astype(BF16)

    def down(pair, half):
        rows = h[span(half)]
        return [jnp.dot(rows, wd[2 * pair + i], preferred_element_type=F32) for i in range(2)]

    def down_cross_send(k, half=None):
        for i, term in enumerate(down(0, half)):
            t_send[k, i, span(half)] = term.astype(BF16)
        for i in range(2):
            cross_term(k, i, half).start()

    def down_cross(half=None):
        for i, term in enumerate(down(1, half)):
            cross[i, span(half)] = term

    def down_own_send(k, half=None):
        for i, term in enumerate(down(2, half)):
            t_send[k, 2 + i, span(half)] = term.astype(BF16)
        own_term(k, half).start()

    def down_own(k, half=None):
        for i, term in enumerate(down(3, half)):
            own[lax.rem(k, 2), i, span(half)] = term

    def wait_d(pair):
        drain(wd.at[pl.ds(2 * pair, 2)], d_sem.at[pair])

    load_x(0).wait()
    for j in range(tiles):
        wait_w(j)
        if j + AHEAD < tiles:
            start_w(j + AHEAD)
        else:
            for u in range(2 * (j + AHEAD - tiles), 2 * (j + AHEAD - tiles) + 2):
                load_d(u).start()
        hidden(0, j, 0)
    pl.semaphore_wait(barrier, 2)
    for u in range(2 * AHEAD, 8):
        load_d(u).start()
    load_x(1).start()
    wait_d(0)
    down_cross_send(0, 0)
    wait_d(1)
    down_cross(0)
    for i in range(2):
        send_cross(0, i, 0)
    wait_d(2)
    down_own_send(0, 0)
    wait_d(3)
    down_own(0, 0)

    for j in range(tiles):
        hidden(0, j, 1)
    finish(0, 0, 0)
    down_cross_send(0, 1)
    down_cross(1)
    down_own_send(0, 1)
    for i in range(2):
        send_cross(0, i, 1)
    down_own(0, 1)
    finish(0, 1, 0)

    @pl.loop(1, n)
    def _(k):
        @pl.when(k + 1 < n)
        def _():
            load_x(k + 1).start()

        load_x(k).wait()
        for j in range(tiles):
            hidden(k, j, None)

        @pl.when(k == 1)
        def _():
            for i in range(2):
                finish(0, i, 1)

        @pl.when(k == 2)
        def _():
            finish(1, 0)

        down_cross_send(k)
        down_cross()
        down_own_send(k)
        down_own(k)
        for i in range(2):
            send_cross(k, i)

        @pl.when(k > 2)
        def _():
            finish(k - 1, 0)

        @pl.when(k > 1)
        def _():
            finish(k - 1, 1)

    for i in range(2):
        finish(n - 1, i)

    bulk = at(y, 0, column(c, 1 - a, 0), n - LAST, 2)
    drain(bulk, agr_sem.at[0])
    pass_copy(0, 0, n - LAST, 2).start()
    for k in range(n - LAST, n):
        for i in range(2):
            ag_copy(k, i).wait_recv()
            pass_copy(k, i).start()

    drain(t_send, ts_sem)
    drain(rs_send, rss_sem)
    mine = at(y, 0, column(c, a, 0), n, 2)
    drain(mine, ags_sem)
    drain(mine, fs_sem)
    drain(at(y, 0, column(c, 1 - a, 0), n, 2), gs_sem)
    drain(at(y, 0, column(1 - c, 0, 0), n, 4), yr_sem)


def solution(mesh):
    def step(x, w_gate, w_up, w_down):
        rows, d = x.shape
        ff = w_gate.shape[1]
        n, tiles = rows // R, ff // C
        dma = pltpu.SemaphoreType.DMA
        return pl.pallas_call(
            functools.partial(kernel, n),
            out_shape=pltpu.VMEM((rows, d), BF16),
            in_specs=[pl.BlockSpec(memory_space=pltpu.HBM)] * 4,
            out_specs=pl.BlockSpec(memory_space=pltpu.VMEM),
            scratch_shapes=[
                pltpu.VMEM((2, R, d), BF16),
                pltpu.VMEM((tiles, 2, d, C), BF16),
                pltpu.VMEM((8, ff, C), BF16),
                pltpu.VMEM((R, ff), BF16),
                pltpu.VMEM((n, 4, R, C), BF16),
                pltpu.VMEM((n, 4, R, C), BF16),
                pltpu.VMEM((2, R, C), F32),
                pltpu.VMEM((n, 2, R, C), BF16),
                pltpu.VMEM((n, 2, R, C), BF16),
                pltpu.VMEM((2, 2, R, C), F32),
                dma((2,)), dma((AHEAD,)), dma((4,)), dma(()), dma((5, 2)), dma((5,)), dma(()), dma((5, 2)),
                dma(()), dma((1 + 2 * LAST,)), dma(()), dma(()), dma(()),
            ],
            compiler_params=pltpu.CompilerParams(
                collective_id=0, has_side_effects=True, vmem_limit_bytes=52 * 2**20
            ),
            cost_estimate=pl.CostEstimate(
                flops=6 * rows * d * ff, bytes_accessed=2 * (2 * rows * d + 3 * d * ff), transcendentals=rows * ff
            ),
        )(x, w_gate, w_up, w_down)

    return jax.shard_map(
        step,
        mesh=mesh,
        in_specs=(P("dp", None), P(None, "tp"), P(None, "tp"), P("tp", None)),
        out_specs=P("dp", None),
        check_vma=False,
    )
```

```python
import functools

import jax
import jax.numpy as jnp
from jax import lax
from jax.experimental import pallas as pl
from jax.experimental.pallas import tpu as pltpu
from jax.sharding import PartitionSpec as P

MESH = pl.DeviceIdType.MESH
BF16, F32 = jnp.bfloat16, jnp.float32
R = 256
H = R // 2
C = 256
AHEAD = 3
LAST = 2


def kernel(
    n, x_hbm, wg_hbm, wu_hbm, wd_hbm, y, xb, wgu, wd, h, t_send, t_recv, cross, rs_send, rs_recv, own,
    x_sem, w_sem, d_sem, ts_sem, tr_sem, ta_sem, rss_sem, rsr_sem, ags_sem, agr_sem, fs_sem, gs_sem, yr_sem,
):
    me = lax.axis_index("tp")
    a, c = me // 2, lax.rem(me, 2)
    sib = {"tp": me + 1 - 2 * c}
    across = {"tp": lax.rem(me + 2, 4)}
    tiles = wgu.shape[0]
    rows = n * R

    def column(half, quarter, i):
        return pl.multiple_of(half * 4 * C + quarter * 2 * C + i * C, C)

    def span(half):
        return pl.ds(0, R) if half is None else pl.ds(half * H, H)

    def slot_of(k, half):
        return 4 if half == 1 else lax.rem(k, 4)

    def tile(k, i, half):
        first, count = (0, R) if half is None else (half * H, H)
        return pl.ds(pl.multiple_of(k * R + first, H), count), pl.ds(column(c, a, i), C)

    def at(ref, k, col, chunks=1, wide=1):
        return ref.at[pl.ds(pl.multiple_of(k * R, R), chunks * R), pl.ds(col, wide * C)]

    def load_x(k):
        return pltpu.make_async_copy(
            x_hbm.at[pl.ds(pl.multiple_of(k * R, R), R), :], xb.at[lax.rem(k, 2)], x_sem.at[lax.rem(k, 2)]
        )

    def start_w(j):
        for m, w in enumerate((wg_hbm, wu_hbm)):
            pltpu.make_async_copy(w.at[:, pl.ds(j * C, C)], wgu.at[j, m], w_sem.at[j % AHEAD]).start(priority=1 if j else 0)

    def wait_w(j):
        pltpu.make_async_copy(wgu.at[j], wgu.at[j], w_sem.at[j % AHEAD]).wait()

    def load_d(u):
        half = 1 - c if u % 4 < 2 else c
        col = column(half, 1 - a if u < 4 else a, u % 2)
        return pltpu.make_async_copy(wd_hbm.at[:, pl.ds(col, C)], wd.at[u], d_sem.at[u // 2])

    def remote(src, dst, ssem, rsem, to):
        return pltpu.make_async_remote_copy(src, dst, ssem, rsem, device_id=to, device_id_type=MESH)

    def cross_term(k, i, half):
        part = span(half)
        return remote(
            t_send.at[k, i, part], t_recv.at[k, i, part], ts_sem, tr_sem.at[slot_of(k, half), i], sib
        )

    def own_term(k, half):
        two, part = pl.ds(2, 2), span(half)
        return remote(
            t_send.at[k, two, part], t_recv.at[k, two, part], ts_sem, ta_sem.at[slot_of(k, half)], sib
        )

    def rs_copy(k, i, half):
        part = span(half)
        return remote(
            rs_send.at[k, i, part], rs_recv.at[k, i, part], rss_sem, rsr_sem.at[slot_of(k, half), i], across
        )

    def ag_copy(k, i, half=None):
        part = y.at[tile(k, i, half)]
        slot = k // (n - LAST) * (1 + 2 * (k - (n - LAST)) + i)
        return remote(part, part, ags_sem, agr_sem.at[slot], across)

    def own_copy(k, i, half):
        part = y.at[tile(k, i, half)]
        return remote(part, part, fs_sem, yr_sem, sib)

    def pass_copy(k, i, chunks=1, wide=1):
        part = at(y, k, column(c, 1 - a, i), chunks, wide)
        return remote(part, part, gs_sem, yr_sem, sib)

    def drain(ref, sem):
        pltpu.make_async_copy(ref, ref, sem).wait()

    load_x(0).start()
    for j in range(AHEAD):
        start_w(j)
    barrier = pltpu.get_barrier_semaphore()
    for to in (sib, across):
        pl.semaphore_signal(barrier, inc=1, device_id=to, device_id_type=MESH)

    def send_cross(k, i, half=None):
        part = span(half)
        cross_term(k, i, half).wait_recv()
        rs_send[k, i, part] = (cross[i, part] + t_recv[k, i, part].astype(F32)).astype(BF16)
        rs_copy(k, i, half).start()

    def finish(k, i, half=None):
        part = span(half)
        if i == 0 and half != 1:
            own_term(k, None).wait_recv()
        rs_copy(k, i, half).wait_recv()
        total = own[lax.rem(k, 2), i, part] + t_recv[k, 2 + i, part].astype(F32) + rs_recv[k, i, part].astype(F32)
        y[tile(k, i, half)] = total.astype(BF16)
        ag_copy(k, i, half).start()
        own_copy(k, i, half).start()

    def hidden(k, j, half):
        slot, part = lax.rem(k, 2), span(half)
        rows = xb[slot, part]
        gate = jnp.dot(rows, wgu[j, 0], preferred_element_type=F32)
        up = jnp.dot(rows, wgu[j, 1], preferred_element_type=F32)
        h[part, pl.ds(j * C, C)] = (jax.nn.silu(gate) * up).astype(BF16)

    def down(pair, half):
        rows = h[span(half)]
        return [jnp.dot(rows, wd[2 * pair + i], preferred_element_type=F32) for i in range(2)]

    def down_cross_send(k, half=None):
        for i, term in enumerate(down(0, half)):
            t_send[k, i, span(half)] = term.astype(BF16)
        for i in range(2):
            cross_term(k, i, half).start()

    def down_cross(half=None):
        for i, term in enumerate(down(1, half)):
            cross[i, span(half)] = term

    def down_own_send(k, half=None):
        for i, term in enumerate(down(2, half)):
            t_send[k, 2 + i, span(half)] = term.astype(BF16)
        own_term(k, half).start()

    def down_own(k, half=None):
        for i, term in enumerate(down(3, half)):
            own[lax.rem(k, 2), i, span(half)] = term

    def wait_d(pair):
        drain(wd.at[pl.ds(2 * pair, 2)], d_sem.at[pair])

    load_x(0).wait()
    for j in range(tiles):
        wait_w(j)
        if j + AHEAD < tiles:
            start_w(j + AHEAD)
        else:
            for u in range(2 * (j + AHEAD - tiles), 2 * (j + AHEAD - tiles) + 2):
                load_d(u).start()
        hidden(0, j, 0)
    pl.semaphore_wait(barrier, 2)
    for u in range(2 * AHEAD, 8):
        load_d(u).start()
    load_x(1).start()
    wait_d(0)
    down_cross_send(0, 0)
    wait_d(1)
    down_cross(0)
    for i in range(2):
        send_cross(0, i, 0)

    for j in range(tiles):
        hidden(0, j, 1)
    down_cross_send(0, 1)
    down_cross(1)
    wait_d(2)
    down_own_send(0)
    for i in range(2):
        send_cross(0, i, 1)
    wait_d(3)
    down_own(0)
    for i in range(2):
        finish(0, i, 0)

    @pl.loop(1, n)
    def _(k):
        @pl.when(k + 1 < n)
        def _():
            load_x(k + 1).start()

        load_x(k).wait()
        for j in range(tiles):
            hidden(k, j, None)

        @pl.when(k == 1)
        def _():
            for i in range(2):
                finish(0, i, 1)

        @pl.when(k == 2)
        def _():
            finish(1, 0)

        down_cross_send(k)
        down_cross()
        down_own_send(k)
        down_own(k)
        for i in range(2):
            send_cross(k, i)

        @pl.when(k > 2)
        def _():
            finish(k - 1, 0)

        @pl.when(k > 1)
        def _():
            finish(k - 1, 1)

    for i in range(2):
        finish(n - 1, i)

    bulk = at(y, 0, column(c, 1 - a, 0), n - LAST, 2)
    drain(bulk, agr_sem.at[0])
    pass_copy(0, 0, n - LAST, 2).start()
    for k in range(n - LAST, n):
        for i in range(2):
            ag_copy(k, i).wait_recv()
            pass_copy(k, i).start()

    drain(t_send, ts_sem)
    drain(rs_send, rss_sem)
    mine = at(y, 0, column(c, a, 0), n, 2)
    drain(mine, ags_sem)
    drain(mine, fs_sem)
    drain(at(y, 0, column(c, 1 - a, 0), n, 2), gs_sem)
    drain(at(y, 0, column(1 - c, 0, 0), n, 4), yr_sem)


def solution(mesh):
    def step(x, w_gate, w_up, w_down):
        rows, d = x.shape
        ff = w_gate.shape[1]
        n, tiles = rows // R, ff // C
        dma = pltpu.SemaphoreType.DMA
        return pl.pallas_call(
            functools.partial(kernel, n),
            out_shape=pltpu.VMEM((rows, d), BF16),
            in_specs=[pl.BlockSpec(memory_space=pltpu.HBM)] * 4,
            out_specs=pl.BlockSpec(memory_space=pltpu.VMEM),
            scratch_shapes=[
                pltpu.VMEM((2, R, d), BF16),
                pltpu.VMEM((tiles, 2, d, C), BF16),
                pltpu.VMEM((8, ff, C), BF16),
                pltpu.VMEM((R, ff), BF16),
                pltpu.VMEM((n, 4, R, C), BF16),
                pltpu.VMEM((n, 4, R, C), BF16),
                pltpu.VMEM((2, R, C), F32),
                pltpu.VMEM((n, 2, R, C), BF16),
                pltpu.VMEM((n, 2, R, C), BF16),
                pltpu.VMEM((2, 2, R, C), F32),
                dma((2,)), dma((AHEAD,)), dma((4,)), dma(()), dma((5, 2)), dma((5,)), dma(()), dma((5, 2)),
                dma(()), dma((1 + 2 * LAST,)), dma(()), dma(()), dma(()),
            ],
            compiler_params=pltpu.CompilerParams(
                collective_id=0, has_side_effects=True, vmem_limit_bytes=52 * 2**20
            ),
            cost_estimate=pl.CostEstimate(
                flops=6 * rows * d * ff, bytes_accessed=2 * (2 * rows * d + 3 * d * ff), transcendentals=rows * ff
            ),
        )(x, w_gate, w_up, w_down)

    return jax.shard_map(
        step,
        mesh=mesh,
        in_specs=(P("dp", None), P(None, "tp"), P(None, "tp"), P("tp", None)),
        out_specs=P("dp", None),
        check_vma=False,
    )
```
